32 devices in a mesh: batch: 1 (over z), col: 4 (over y), row: 8 (over x, core).
Axes of the slice: x: 4, y: 4, z: 1, core: 2. Of those that a mesh axis runs over, the one named last changes fastest.
The devices are a block of a 4x4x8 slice.
Arguments:
- z_one: bfloat16 [1024, 1024, 128], P(('batch', 'row'), 'col')
- z_two: bfloat16 [1024, 1024, 128], P(('batch', 'row'), 'col')
- mask_one: int32 [1024, 1024], P(('batch', 'row'), 'col')
- mask_two: int32 [1024, 1024], P(('batch', 'row'), 'col')
- ln_in_scale: bfloat16 [128], replicated
- w_a: bfloat16 [128, 128], replicated
- w_a_gate: bfloat16 [128, 128], replicated
- w_b: bfloat16 [128, 128], replicated
- w_b_gate: bfloat16 [128, 128], replicated
- w_gate: bfloat16 [128, 128], replicated
- w_out: bfloat16 [128, 128], replicated
- ln_out_scale: bfloat16 [128], replicated
Outputs:
- output 1: bfloat16 [1024, 1024, 128], P(('batch', 'row'), 'col')
- output 2: bfloat16 [1024, 1024, 128], P(('batch', 'row'), 'col')
All inputs are finite; a program needn't handle non-finite values.
Results may differ from the reference program's by a relative error of at most 0.00127835.
Values are sent between devices in bfloat16 or wider.
A program may use at most 768 MiB of HBM per device.

```python
import jax
import jax.numpy as jnp
from jax import lax

NRES = 1024
CZ = 128
CHID = 128
ROW_BLOCK = 128


def layer_norm(values, scale):
    row_mean = jnp.mean(values, axis=-1, keepdims=True)
    centered = values - row_mean
    variance = jnp.mean(centered * centered, axis=-1, keepdims=True)
    return centered * lax.rsqrt(variance + 1e-5) * scale.astype(jnp.float32)


def linear(normed, weight):
    flat = normed.reshape(-1, normed.shape[-1])
    result = jnp.dot(flat, weight, preferred_element_type=jnp.float32)
    return result.reshape(normed.shape[:-1] + (weight.shape[1],))


def one_crop(pair, mask, ln_in_scale, w_a, w_a_gate, w_b, w_b_gate, w_gate, w_out, ln_out_scale):
    block_count = NRES // ROW_BLOCK
    pair_blocks = pair.reshape(block_count, ROW_BLOCK, NRES, CZ)
    mask_blocks = mask.reshape(block_count, ROW_BLOCK, NRES)

    def project(block):
        pair_blk, mask_blk = block
        normed = layer_norm(pair_blk.astype(jnp.float32), ln_in_scale).astype(jnp.bfloat16)
        mask_val = mask_blk.astype(jnp.float32)[:, :, None]
        left = mask_val * jax.nn.sigmoid(linear(normed, w_a_gate)) * linear(normed, w_a)
        right = mask_val * jax.nn.sigmoid(linear(normed, w_b_gate)) * linear(normed, w_b)
        return left.astype(jnp.bfloat16), right.astype(jnp.bfloat16)

    left_all, right_all = lax.map(project, (pair_blocks, mask_blocks))
    right_major = jnp.transpose(right_all.reshape(NRES, NRES, CHID).astype(jnp.float32), (2, 0, 1))

    def finish(block):
        pair_blk, left_blk = block
        normed = layer_norm(pair_blk.astype(jnp.float32), ln_in_scale).astype(jnp.bfloat16)
        gate = jax.nn.sigmoid(linear(normed, w_gate))
        left_major = jnp.transpose(left_blk.astype(jnp.float32), (2, 0, 1))
        contracted = jnp.einsum('cik,cjk->ijc', left_major, right_major)
        normed_out = layer_norm(contracted, ln_out_scale).astype(jnp.bfloat16)
        update = linear(normed_out, w_out)
        return (pair_blk.astype(jnp.float32) + gate * update).astype(jnp.bfloat16)

    out_blocks = lax.map(finish, (pair_blocks, left_all))
    return out_blocks.reshape(NRES, NRES, CZ)


def setup_inputs(seed: int = 0, part: int = 0) -> dict:
    root = jax.random.key(seed)
    shared_key, crop_base = jax.random.split(root)
    crop_keys = jax.random.split(jax.random.fold_in(crop_base, part), 4)
    weight_keys = jax.random.split(shared_key, 8)

    def pair_draw(key_in):
        return jax.random.normal(key_in, (NRES, NRES, CZ), jnp.float32).astype(jnp.bfloat16)

    def mask_draw(key_in):
        valid = (jax.random.randint(key_in, (NRES,), 0, 10) != 0).astype(jnp.int32)
        return valid[:, None] * valid[None, :]

    def weight_draw(key_in, fan_in, fan_out):
        values = jax.random.normal(key_in, (fan_in, fan_out), jnp.float32) * fan_in ** -0.5
        return values.astype(jnp.bfloat16)

    def scale_draw(key_in, width):
        return jax.random.uniform(key_in, (width,), jnp.float32, 0.5, 1.5).astype(jnp.bfloat16)

    return {
        'z_one': pair_draw(crop_keys[0]),
        'z_two': pair_draw(crop_keys[1]),
        'mask_one': mask_draw(crop_keys[2]),
        'mask_two': mask_draw(crop_keys[3]),
        'ln_in_scale': scale_draw(weight_keys[0], CZ),
        'w_a': weight_draw(weight_keys[1], CZ, CHID),
        'w_a_gate': weight_draw(weight_keys[2], CZ, CHID),
        'w_b': weight_draw(weight_keys[3], CZ, CHID),
        'w_b_gate': weight_draw(weight_keys[4], CZ, CHID),
        'w_gate': weight_draw(weight_keys[5], CZ, CZ),
        'w_out': weight_draw(weight_keys[6], CHID, CZ),
        'ln_out_scale': scale_draw(weight_keys[7], CHID),
    }


def reference(z_one, z_two, mask_one, mask_two, ln_in_scale, w_a, w_a_gate, w_b, w_b_gate, w_gate, w_out, ln_out_scale):
    out_one = one_crop(z_one, mask_one, ln_in_scale, w_a, w_a_gate, w_b, w_b_gate, w_gate, w_out, ln_out_scale)
    out_two = one_crop(z_two, mask_two, ln_in_scale, w_a, w_a_gate, w_b, w_b_gate, w_gate, w_out, ln_out_scale)
    return (out_one, out_two)
```

```python
import functools
import jax
import jax.numpy as jnp
from jax import lax
from jax.experimental import pallas as pl
from jax.experimental.pallas import tpu as pltpu
from jax.sharding import PartitionSpec as P

F32 = jnp.float32
BF16 = jnp.bfloat16
CORES = 2
VMEM_LIMIT = 56 << 20


def sigmoid(values):
    return 0.5 * jnp.tanh(0.5 * values) + 0.5


def params():
    return pltpu.CompilerParams(vmem_limit_bytes=VMEM_LIMIT)


def cost(flops, moved):
    return pl.CostEstimate(flops=int(flops), bytes_accessed=int(moved), transcendentals=0)


def project_kernel(z_ref, mask_ref, weight_ref, scale_ref, *outs, row_block, col_count):
    a_refs, b_refs, normed_ref = outs[:col_count], outs[col_count:-1], outs[-1]
    scale = scale_ref[...].astype(F32)
    ch = weight_ref.shape[0] // 4
    lefts, rights = [], []
    for r in range(row_block):
        values = z_ref[r].astype(F32)
        centered = values - jnp.mean(values, axis=-1, keepdims=True)
        variance = jnp.mean(centered * centered, axis=-1, keepdims=True)
        normed = (centered * lax.rsqrt(variance + 1e-5) * scale).astype(BF16)
        normed_ref[r] = normed
        proj = lax.dot_general(weight_ref[...], normed, (((1,), (1,)), ((), ())), preferred_element_type=F32)
        mask = mask_ref[r:r + 1, :].astype(F32)
        lefts.append((mask * sigmoid(proj[ch:2 * ch]) * proj[:ch]).astype(BF16))
        rights.append((mask * sigmoid(proj[3 * ch:]) * proj[2 * ch:3 * ch]).astype(BF16))
    left = jnp.swapaxes(jnp.stack(lefts), 0, 1)
    right = jnp.swapaxes(jnp.stack(rights), 0, 1)
    for refs, arr in ((a_refs, left), (b_refs, right)):
        part = ch // len(refs)
        for n, ref in enumerate(refs):
            ref[...] = arr[n * part:(n + 1) * part]


def project(z, mask, weight, scale, col_count, row_block=16):
    rows, cols, dim = z.shape
    ch = weight.shape[0] // 4
    parts = [ch // col_count] * col_count + [ch // (col_count * CORES)] * (col_count * CORES)
    return pl.pallas_call(
        functools.partial(project_kernel, row_block=row_block, col_count=col_count),
        grid=(rows // row_block,),
        in_specs=[
            pl.BlockSpec((row_block, cols, dim), lambda i: (i, 0, 0)),
            pl.BlockSpec((row_block, cols), lambda i: (i, 0)),
            pl.BlockSpec(weight.shape, lambda i: (0, 0)),
            pl.BlockSpec(scale.shape, lambda i: (0, 0)),
        ],
        out_specs=[pl.BlockSpec((p, row_block, cols), lambda i: (0, i, 0)) for p in parts]
        + [pl.BlockSpec((row_block, cols, dim), lambda i: (i, 0, 0))],
        out_shape=[jax.ShapeDtypeStruct((p, rows, cols), BF16) for p in parts]
        + [jax.ShapeDtypeStruct((rows, cols, dim), BF16)],
        compiler_params=params(),
        cost_estimate=cost(2 * rows * cols * dim * ch * 4, rows * cols * dim * 8),
        name="project",
    )(z, mask, weight, scale)


def contract_kernel(col_ref, inv_ref, *refs, piece_count, col_count, ch_block, first):
    a_refs = refs[:col_count]
    b_refs = refs[col_count:col_count + piece_count]
    prev_ref = None if first else refs[col_count + piece_count]
    o_ref, stat_ref = refs[-2:]
    step, target = pl.program_id(0), pl.program_id(1)
    if first:
        @pl.when(step == 0)
        def _():
            stat_ref[target] = jnp.zeros(stat_ref.shape[1:], F32)
    else:
        @pl.when(step == 0)
        def _():
            stat_ref[target] = prev_ref[target]
    mean, m2 = stat_ref[target, 0], stat_ref[target, 1]
    for c in range(ch_block):
        a_row = jnp.concatenate([ref[c] for ref in a_refs], axis=1)
        b_row = jnp.concatenate([ref[0, k, c] for ref in b_refs for k in range(ref.shape[1])], axis=1)
        out = lax.dot_general(a_row, b_row, (((1,), (1,)), ((), ())), preferred_element_type=F32)
        o_ref[0, c] = out
        delta = out - mean
        mean = mean + delta * inv_ref[step * ch_block + c]
        m2 = m2 + delta * (out - mean)
    stat_ref[target, 0] = mean
    stat_ref[target, 1] = m2


def contract(col, inv, a_parts, b_pieces, prev, half, ch_block=4):
    rows, cols = a_parts[0].shape[1:]
    col_count = len(a_parts)
    part, width = b_pieces[0].shape[2:4]
    first = prev is None
    stat_shape = (col_count, 2, rows, width)
    a_off = half * (part // ch_block)
    in_specs = [pl.BlockSpec((ch_block, rows, cols), lambda c, t, col: (a_off + c, 0, 0)) for _ in a_parts]
    for piece in b_pieces:
        in_specs.append(pl.BlockSpec(
            (1, piece.shape[1], ch_block, width, cols),
            lambda c, t, col: (lax.rem(col[0] + t, col_count), 0, c, 0, 0)))
    args = [*a_parts, *b_pieces]
    if not first:
        in_specs.append(pl.BlockSpec(stat_shape, lambda c, t, col: (0, 0, 0, 0)))
        args.append(prev)
    return pl.pallas_call(
        functools.partial(contract_kernel, piece_count=len(b_pieces), col_count=col_count, ch_block=ch_block, first=first),
        grid_spec=pltpu.PrefetchScalarGridSpec(
            num_scalar_prefetch=1,
            grid=(part // ch_block, col_count),
            in_specs=[pl.BlockSpec(memory_space=pltpu.SMEM)] + in_specs,
            out_specs=[
                pl.BlockSpec((1, ch_block, rows, width), lambda c, t, col: (t, c, 0, 0)),
                pl.BlockSpec(stat_shape, lambda c, t, col: (0, 0, 0, 0)),
            ],
        ),
        out_shape=[
            jax.ShapeDtypeStruct((col_count, part, rows, width), F32),
            jax.ShapeDtypeStruct(stat_shape, F32),
        ],
        compiler_params=params(),
        cost_estimate=cost(2 * part * rows * width * col_count * cols * col_count, part * width * cols * col_count * col_count * 2),
        name="contract",
    )(col, inv, *args)


def normalize_kernel(scale_ref, own_ref, sib_ref, *refs, total_ch):
    stat_refs, out_ref = refs[:-1], refs[-1]
    means = [ref[0, 0] for ref in stat_refs]
    count = len(stat_refs)
    group = total_ch // count
    mean = sum(means[1:], means[0]) * (1.0 / count)
    m2 = sum([ref[0, 1] for ref in stat_refs[1:]], stat_refs[0][0, 1])
    spread = sum([(m - mean) * (m - mean) for m in means[1:]], (means[0] - mean) * (means[0] - mean))
    rstd = lax.rsqrt((m2 + group * spread) * (1.0 / total_ch) + 1e-5)
    part = own_ref.shape[1]
    for n, ref in enumerate((own_ref, sib_ref)):
        for c in range(part):
            out_ref[n * part + c] = ((ref[0, c] - mean) * rstd * scale_ref[n * part + c]).astype(BF16)


def normalize(scale, own, sib, stats, target, total_ch, row_block=32):
    col_count, part, rows, width = own.shape
    o_spec = pl.BlockSpec((1, part, row_block, width), lambda i: (target, 0, i, 0))

    def stat_spec(index):
        return pl.BlockSpec((1, 2, row_block, width), lambda i: (index, 0, i, 0))

    return pl.pallas_call(
        functools.partial(normalize_kernel, total_ch=total_ch),
        grid=(rows // row_block,),
        in_specs=[pl.BlockSpec(memory_space=pltpu.SMEM), o_spec, o_spec]
        + [stat_spec((target + e) % col_count) for e in range(col_count)],
        out_specs=pl.BlockSpec((2 * part, row_block, width), lambda i: (0, i, 0)),
        out_shape=jax.ShapeDtypeStruct((2 * part, rows, width), BF16),
        compiler_params=params(),
        cost_estimate=cost(2 * part * rows * width * 1000, part * rows * width * 12),
        name="normalize",
    )(scale, own, sib, *stats)


def finish_kernel(normed_ref, z_ref, w_out_ref, w_gate_ref, *refs, row_block, chunks, col_count, half_cols):
    out_ref = refs[-1]
    tiles = []
    for q in range(len(chunks)):
        group = refs[q * col_count:(q + 1) * col_count]
        tiles.append(jnp.concatenate([jnp.swapaxes(ref[...], 0, 1) for ref in group], axis=1))
    for r in range(row_block):
        gate = sigmoid(jnp.dot(normed_ref[r], w_gate_ref[...], preferred_element_type=F32))
        for tile, (start, size) in zip(tiles, chunks):
            update = lax.dot_general(tile[r], w_out_ref[...], (((0,), (0,)), ((), ())), preferred_element_type=F32)
            for core in range(CORES):
                lo = core * half_cols + start
                new = z_ref[r, lo:lo + size].astype(F32) + gate[lo:lo + size] * update[core * size:(core + 1) * size]
                out_ref[r, lo:lo + size] = new.astype(BF16)


def finish(normed, z, w_out, w_gate, chunk_parts, chunks, row_block=16):
    rows, cols, dim = z.shape
    row_spec = pl.BlockSpec((row_block, cols, dim), lambda i: (i, 0, 0))
    w_spec = pl.BlockSpec(w_out.shape, lambda i: (0, 0))
    flat = [arr for parts in chunk_parts for arr in parts]
    return pl.pallas_call(
        functools.partial(finish_kernel, row_block=row_block, chunks=chunks, col_count=len(chunk_parts[0]), half_cols=cols // CORES),
        grid=(rows // row_block,),
        in_specs=[row_spec, row_spec, w_spec, w_spec]
        + [pl.BlockSpec((arr.shape[0], row_block, arr.shape[2]), lambda i: (0, i, 0)) for arr in flat],
        out_specs=row_spec,
        out_shape=jax.ShapeDtypeStruct(z.shape, BF16),
        compiler_params=params(),
        cost_estimate=cost(4 * rows * cols * dim * dim, rows * cols * dim * 8),
        name="finish",
    )(normed, z, w_out, w_gate, *flat)


def solution(mesh):
    row_count = mesh.shape['row']
    col_count = mesh.shape['col']
    chip_rows = row_count // CORES
    chip_groups = [[x * CORES + core for x in range(chip_rows)] for core in range(CORES)]
    pair_spec = P(('batch', 'row'), 'col', None)
    mask_spec = P(('batch', 'row'), 'col')
    replicated = P()

    def along_col(arr, shift):
        return lax.ppermute(arr, 'col', [(s, (s + shift) % col_count) for s in range(col_count)])

    def along_col_swapped(arr, shift):
        return lax.ppermute(arr, ('col', 'row'), [
            (s * row_count + r, ((s + shift) % col_count) * row_count + (r ^ 1))
            for s in range(col_count) for r in range(row_count)])

    def core_swap(arr):
        return lax.ppermute(arr, 'row', [(r, r ^ 1) for r in range(row_count)])

    def device_fn(z_one, z_two, mask_one, mask_two, ln_in_scale, w_a, w_a_gate, w_b, w_b_gate, w_gate, w_out, ln_out_scale):
        col = lax.axis_index('col')
        core = lax.rem(lax.axis_index('row'), CORES)
        hidden = w_out.shape[0]
        rows_loc = z_one.shape[0]

        def group_order(arr, sign):
            part = hidden // (col_count * CORES)
            grouped = arr.reshape((col_count, CORES, part) + arr.shape[1:])
            order = lax.rem(col + sign * jnp.arange(col_count) + col_count, col_count)
            grouped = jnp.take(grouped, order, axis=0)
            return jnp.where(core == 0, grouped, grouped[:, ::-1]).reshape(arr.shape)

        weight = jnp.concatenate([group_order(w.T, 1) for w in (w_a, w_a_gate, w_b, w_b_gate)], axis=0)
        w_back = group_order(w_out, -1)
        scale_own = group_order(ln_out_scale.astype(F32), 1)[:hidden // col_count]
        scale_in = ln_in_scale.reshape(1, -1)
        col_arr = col.reshape(1).astype(jnp.int32)
        inv = 1.0 / (jnp.arange(hidden // col_count, dtype=F32) + 1.0)
        part = hidden // (col_count * CORES)

        def rows_in_order(own, other):
            return jnp.where(core == 0, jnp.concatenate([own, other], axis=1), jnp.concatenate([other, own], axis=1))

        def crop(z, mask, chunks, piece_groups):
            outs = project(z, mask, weight, scale_in, col_count)
            a_send, b_send, normed = outs[:col_count], outs[col_count:-1], outs[-1]
            b_own = [b_send[CORES * d] if d == 0 else along_col(b_send[CORES * d], d) for d in range(col_count)]
            b_sib = [core_swap(b_send[1]) if d == 0 else along_col_swapped(b_send[CORES * d + 1], d) for d in range(col_count)]
            a_parts = [a_send[0]] + [along_col(a_send[d], d) for d in range(1, col_count)]
            chunk_parts = []
            for start, size in chunks:
                own_pieces = []
                for group in piece_groups:
                    piece = jnp.stack([
                        rows_in_order(b_own[d][:, start:start + size], b_sib[d][:, start:start + size]) for d in group])
                    own_pieces.append(lax.all_gather(piece, 'row', axis=0, axis_index_groups=chip_groups))
                sib_pieces = [core_swap(piece) for piece in own_pieces]
                o_own, stat = contract(col_arr, inv[:part], a_parts, own_pieces, None, 0)
                o_sib, stat = contract(col_arr, inv[part:], a_parts, sib_pieces, stat, 1)
                stats = [stat] + [along_col(stat, d) for d in range(1, col_count)]
                parts = []
                for d in range(col_count):
                    result = normalize(scale_own, o_own, o_sib, stats, d, hidden)
                    parts.append(result if d == 0 else along_col(result, d))
                chunk_parts.append(parts)
            return finish(normed, z, w_back, w_gate, chunk_parts, chunks)

        half = rows_loc // 2
        first, rest = [0], list(range(1, col_count))
        out_one = crop(z_one, mask_one, [(0, rows_loc)], [first, rest])
        out_two = crop(z_two, mask_two, [(0, half), (half, half)], [first + rest])
        return out_one, out_two

    return jax.shard_map(
        device_fn,
        mesh=mesh,
        in_specs=(pair_spec, pair_spec, mask_spec, mask_spec, replicated, replicated, replicated, replicated, replicated, replicated, replicated, replicated),
        out_specs=(pair_spec, pair_spec),
        check_vma=False,
    )
```

```python
import functools
import jax
import jax.numpy as jnp
from jax import lax
from jax.experimental import pallas as pl
from jax.experimental.pallas import tpu as pltpu
from jax.sharding import PartitionSpec as P

F32 = jnp.float32
BF16 = jnp.bfloat16
CORES = 2
VMEM_LIMIT = 56 << 20


def sigmoid(values):
    return 0.5 * jnp.tanh(0.5 * values) + 0.5


def params():
    return pltpu.CompilerParams(vmem_limit_bytes=VMEM_LIMIT)


def cost(flops, moved):
    return pl.CostEstimate(flops=int(flops), bytes_accessed=int(moved), transcendentals=0)


def project_kernel(z_ref, mask_ref, weight_ref, scale_ref, *outs, row_block, col_count):
    a_refs, b_refs, normed_ref = outs[:col_count], outs[col_count:-1], outs[-1]
    scale = scale_ref[...].astype(F32)
    ch = weight_ref.shape[0] // 4
    lefts, rights = [], []
    for r in range(row_block):
        values = z_ref[r].astype(F32)
        centered = values - jnp.mean(values, axis=-1, keepdims=True)
        variance = jnp.mean(centered * centered, axis=-1, keepdims=True)
        normed = (centered * lax.rsqrt(variance + 1e-5) * scale).astype(BF16)
        normed_ref[r] = normed
        proj = lax.dot_general(weight_ref[...], normed, (((1,), (1,)), ((), ())), preferred_element_type=F32)
        mask = mask_ref[r:r + 1, :].astype(F32)
        lefts.append((mask * sigmoid(proj[ch:2 * ch]) * proj[:ch]).astype(BF16))
        rights.append((mask * sigmoid(proj[3 * ch:]) * proj[2 * ch:3 * ch]).astype(BF16))
    left = jnp.swapaxes(jnp.stack(lefts), 0, 1)
    right = jnp.swapaxes(jnp.stack(rights), 0, 1)
    for refs, arr in ((a_refs, left), (b_refs, right)):
        part = ch // len(refs)
        for n, ref in enumerate(refs):
            ref[...] = arr[n * part:(n + 1) * part]


def project(z, mask, weight, scale, col_count, row_block=16):
    rows, cols, dim = z.shape
    ch = weight.shape[0] // 4
    parts = [ch // col_count] * col_count + [ch // (col_count * CORES)] * (col_count * CORES)
    return pl.pallas_call(
        functools.partial(project_kernel, row_block=row_block, col_count=col_count),
        grid=(rows // row_block,),
        in_specs=[
            pl.BlockSpec((row_block, cols, dim), lambda i: (i, 0, 0)),
            pl.BlockSpec((row_block, cols), lambda i: (i, 0)),
            pl.BlockSpec(weight.shape, lambda i: (0, 0)),
            pl.BlockSpec(scale.shape, lambda i: (0, 0)),
        ],
        out_specs=[pl.BlockSpec((p, row_block, cols), lambda i: (0, i, 0)) for p in parts]
        + [pl.BlockSpec((row_block, cols, dim), lambda i: (i, 0, 0))],
        out_shape=[jax.ShapeDtypeStruct((p, rows, cols), BF16) for p in parts]
        + [jax.ShapeDtypeStruct((rows, cols, dim), BF16)],
        compiler_params=params(),
        cost_estimate=cost(2 * rows * cols * dim * ch * 4, rows * cols * dim * 8),
        name="project",
    )(z, mask, weight, scale)


def contract_kernel(col_ref, inv_ref, *refs, piece_count, col_count, ch_block, first):
    a_refs = refs[:col_count]
    b_refs = refs[col_count:col_count + piece_count]
    prev_ref = None if first else refs[col_count + piece_count]
    o_ref, stat_ref = refs[-2:]
    step, target = pl.program_id(0), pl.program_id(1)
    if first:
        @pl.when(step == 0)
        def _():
            stat_ref[target] = jnp.zeros(stat_ref.shape[1:], F32)
    else:
        @pl.when(step == 0)
        def _():
            stat_ref[target] = prev_ref[target]
    mean, m2 = stat_ref[target, 0], stat_ref[target, 1]
    for c in range(ch_block):
        a_row = jnp.concatenate([ref[c] for ref in a_refs], axis=1)
        b_row = jnp.concatenate([ref[0, k, c] for ref in b_refs for k in range(ref.shape[1])], axis=1)
        out = lax.dot_general(a_row, b_row, (((1,), (1,)), ((), ())), preferred_element_type=F32)
        o_ref[0, c] = out
        delta = out - mean
        mean = mean + delta * inv_ref[step * ch_block + c]
        m2 = m2 + delta * (out - mean)
    stat_ref[target, 0] = mean
    stat_ref[target, 1] = m2


def contract(col, inv, a_parts, b_pieces, prev, half, ch_block=4):
    rows, cols = a_parts[0].shape[1:]
    col_count = len(a_parts)
    part, width = b_pieces[0].shape[2:4]
    first = prev is None
    stat_shape = (col_count, 2, rows, width)
    a_off = half * (part // ch_block)
    in_specs = [pl.BlockSpec((ch_block, rows, cols), lambda c, t, col: (a_off + c, 0, 0)) for _ in a_parts]
    for piece in b_pieces:
        in_specs.append(pl.BlockSpec(
            (1, piece.shape[1], ch_block, width, cols),
            lambda c, t, col: (lax.rem(col[0] + t, col_count), 0, c, 0, 0)))
    args = [*a_parts, *b_pieces]
    if not first:
        in_specs.append(pl.BlockSpec(stat_shape, lambda c, t, col: (0, 0, 0, 0)))
        args.append(prev)
    return pl.pallas_call(
        functools.partial(contract_kernel, piece_count=len(b_pieces), col_count=col_count, ch_block=ch_block, first=first),
        grid_spec=pltpu.PrefetchScalarGridSpec(
            num_scalar_prefetch=1,
            grid=(part // ch_block, col_count),
            in_specs=[pl.BlockSpec(memory_space=pltpu.SMEM)] + in_specs,
            out_specs=[
                pl.BlockSpec((1, ch_block, rows, width), lambda c, t, col: (t, c, 0, 0)),
                pl.BlockSpec(stat_shape, lambda c, t, col: (0, 0, 0, 0)),
            ],
        ),
        out_shape=[
            jax.ShapeDtypeStruct((col_count, part, rows, width), F32),
            jax.ShapeDtypeStruct(stat_shape, F32),
        ],
        compiler_params=params(),
        cost_estimate=cost(2 * part * rows * width * col_count * cols * col_count, part * width * cols * col_count * col_count * 2),
        name="contract",
    )(col, inv, *args)


def normalize_kernel(scale_ref, own_ref, sib_ref, *refs, total_ch):
    stat_refs, out_ref = refs[:-1], refs[-1]
    means = [ref[0, 0] for ref in stat_refs]
    count = len(stat_refs)
    group = total_ch // count
    mean = sum(means[1:], means[0]) * (1.0 / count)
    m2 = sum([ref[0, 1] for ref in stat_refs[1:]], stat_refs[0][0, 1])
    spread = sum([(m - mean) * (m - mean) for m in means[1:]], (means[0] - mean) * (means[0] - mean))
    rstd = lax.rsqrt((m2 + group * spread) * (1.0 / total_ch) + 1e-5)
    part = own_ref.shape[1]
    for n, ref in enumerate((own_ref, sib_ref)):
        for c in range(part):
            out_ref[n * part + c] = ((ref[0, c] - mean) * rstd * scale_ref[n * part + c]).astype(BF16)


def normalize(scale, own, sib, stats, target, total_ch, row_block=32):
    col_count, part, rows, width = own.shape
    o_spec = pl.BlockSpec((1, part, row_block, width), lambda i: (target, 0, i, 0))

    def stat_spec(index):
        return pl.BlockSpec((1, 2, row_block, width), lambda i: (index, 0, i, 0))

    return pl.pallas_call(
        functools.partial(normalize_kernel, total_ch=total_ch),
        grid=(rows // row_block,),
        in_specs=[pl.BlockSpec(memory_space=pltpu.SMEM), o_spec, o_spec]
        + [stat_spec((target + e) % col_count) for e in range(col_count)],
        out_specs=pl.BlockSpec((2 * part, row_block, width), lambda i: (0, i, 0)),
        out_shape=jax.ShapeDtypeStruct((2 * part, rows, width), BF16),
        compiler_params=params(),
        cost_estimate=cost(2 * part * rows * width * 1000, part * rows * width * 12),
        name="normalize",
    )(scale, own, sib, *stats)


def finish_kernel(normed_ref, z_ref, w_out_ref, w_gate_ref, *refs, row_block, chunks, col_count, half_cols):
    out_ref = refs[-1]
    tiles = []
    for q in range(len(chunks)):
        group = refs[q * col_count:(q + 1) * col_count]
        tiles.append(jnp.concatenate([jnp.swapaxes(ref[...], 0, 1) for ref in group], axis=1))
    for r in range(row_block):
        gate = sigmoid(jnp.dot(normed_ref[r], w_gate_ref[...], preferred_element_type=F32))
        for tile, (start, size) in zip(tiles, chunks):
            update = lax.dot_general(tile[r], w_out_ref[...], (((0,), (0,)), ((), ())), preferred_element_type=F32)
            for core in range(CORES):
                lo = core * half_cols + start
                new = z_ref[r, lo:lo + size].astype(F32) + gate[lo:lo + size] * update[core * size:(core + 1) * size]
                out_ref[r, lo:lo + size] = new.astype(BF16)


def finish(normed, z, w_out, w_gate, chunk_parts, chunks, row_block=16):
    rows, cols, dim = z.shape
    row_spec = pl.BlockSpec((row_block, cols, dim), lambda i: (i, 0, 0))
    w_spec = pl.BlockSpec(w_out.shape, lambda i: (0, 0))
    flat = [arr for parts in chunk_parts for arr in parts]
    return pl.pallas_call(
        functools.partial(finish_kernel, row_block=row_block, chunks=chunks, col_count=len(chunk_parts[0]), half_cols=cols // CORES),
        grid=(rows // row_block,),
        in_specs=[row_spec, row_spec, w_spec, w_spec]
        + [pl.BlockSpec((arr.shape[0], row_block, arr.shape[2]), lambda i: (0, i, 0)) for arr in flat],
        out_specs=row_spec,
        out_shape=jax.ShapeDtypeStruct(z.shape, BF16),
        compiler_params=params(),
        cost_estimate=cost(4 * rows * cols * dim * dim, rows * cols * dim * 8),
        name="finish",
    )(normed, z, w_out, w_gate, *flat)


def solution(mesh):
    row_count = mesh.shape['row']
    col_count = mesh.shape['col']
    chip_rows = row_count // CORES
    chip_groups = [[x * CORES + core for x in range(chip_rows)] for core in range(CORES)]
    pair_spec = P(('batch', 'row'), 'col', None)
    mask_spec = P(('batch', 'row'), 'col')
    replicated = P()

    def along_col(arr, shift):
        return lax.ppermute(arr, 'col', [(s, (s + shift) % col_count) for s in range(col_count)])

    def along_col_swapped(arr, shift):
        return lax.ppermute(arr, ('col', 'row'), [
            (s * row_count + r, ((s + shift) % col_count) * row_count + (r ^ 1))
            for s in range(col_count) for r in range(row_count)])

    def core_swap(arr):
        return lax.ppermute(arr, 'row', [(r, r ^ 1) for r in range(row_count)])

    def device_fn(z_one, z_two, mask_one, mask_two, ln_in_scale, w_a, w_a_gate, w_b, w_b_gate, w_gate, w_out, ln_out_scale):
        col = lax.axis_index('col')
        core = lax.rem(lax.axis_index('row'), CORES)
        hidden = w_out.shape[0]
        rows_loc = z_one.shape[0]

        def group_order(arr, sign):
            part = hidden // (col_count * CORES)
            grouped = arr.reshape((col_count, CORES, part) + arr.shape[1:])
            order = lax.rem(col + sign * jnp.arange(col_count) + col_count, col_count)
            grouped = jnp.take(grouped, order, axis=0)
            return jnp.where(core == 0, grouped, grouped[:, ::-1]).reshape(arr.shape)

        weight = jnp.concatenate([group_order(w.T, 1) for w in (w_a, w_a_gate, w_b, w_b_gate)], axis=0)
        w_back = group_order(w_out, -1)
        scale_own = group_order(ln_out_scale.astype(F32), 1)[:hidden // col_count]
        scale_in = ln_in_scale.reshape(1, -1)
        col_arr = col.reshape(1).astype(jnp.int32)
        inv = 1.0 / (jnp.arange(hidden // col_count, dtype=F32) + 1.0)
        part = hidden // (col_count * CORES)

        def rows_in_order(own, other):
            return jnp.where(core == 0, jnp.concatenate([own, other], axis=1), jnp.concatenate([other, own], axis=1))

        def crop(z, mask, chunks, piece_groups):
            outs = project(z, mask, weight, scale_in, col_count)
            a_send, b_send, normed = outs[:col_count], outs[col_count:-1], outs[-1]
            b_sib = [core_swap(b_send[1])]
            b_own = [b_send[0]] + [along_col(b_send[CORES * d], d) for d in range(1, col_count)]
            b_sib += [along_col_swapped(b_send[CORES * d + 1], d) for d in range(1, col_count)]
            a_parts = [a_send[0]] + [along_col(a_send[d], d) for d in range(1, col_count)]
            chunk_parts = []
            for start, size in chunks:
                own_pieces = []
                for group in piece_groups:
                    piece = jnp.stack([
                        rows_in_order(b_own[d][:, start:start + size], b_sib[d][:, start:start + size]) for d in group])
                    own_pieces.append(lax.all_gather(piece, 'row', axis=0, axis_index_groups=chip_groups))
                sib_pieces = []
                for piece in own_pieces:
                    sib_pieces.append(core_swap(piece))
                o_own, stat = contract(col_arr, inv[:part], a_parts, own_pieces, None, 0)
                o_sib, stat = contract(col_arr, inv[part:], a_parts, sib_pieces, stat, 1)
                stats = [stat] + [along_col(stat, d) for d in range(1, col_count)]
                parts = []
                for d in range(col_count):
                    result = normalize(scale_own, o_own, o_sib, stats, d, hidden)
                    parts.append(result if d == 0 else along_col(result, d))
                chunk_parts.append(parts)
            return finish(normed, z, w_back, w_gate, chunk_parts, chunks)

        half = rows_loc // 2
        first, rest = [0], list(range(1, col_count))
        out_one = crop(z_one, mask_one, [(0, rows_loc)], [first, rest])
        out_two = crop(z_two, mask_two, [(0, half), (half, half)], [first + rest])
        return out_one, out_two

    return jax.shard_map(
        device_fn,
        mesh=mesh,
        in_specs=(pair_spec, pair_spec, mask_spec, mask_spec, replicated, replicated, replicated, replicated, replicated, replicated, replicated, replicated),
        out_specs=(pair_spec, pair_spec),
        check_vma=False,
    )
```
